32 devices in a mesh: section: 4 (over y, x), depth: 8 (over z, core).
Axes of the slice: x: 2, y: 2, z: 4, core: 2. Of those that a mesh axis runs over, the one named last changes fastest.
Arguments:
- activations: float32 [4, 4, 16, 64, 256], P('section', None, 'depth'), may hold values from -6 to 6
- filters: float32 [4, 27, 64, 64], P('section'), may hold values from -0.15625 to 0.15625
- cotangent: float32 [4, 16, 64, 256], P(None, 'depth'), may hold values from -6 to 6
Outputs:
- input_grads: float32 [4, 4, 16, 64, 256], P('section', None, 'depth')
- filter_grads: float32 [4, 27, 64, 64], P('section')
The draws below stay inside these ranges and needn't reach their ends.
All inputs are finite; a program needn't handle non-finite values.
Results may differ from the reference program's by a relative error of at most 0.0003.
Values sent between devices are 32-bit elements; how exact they have to be, the bound alone decides.
A program may use at most 128 MiB of HBM per device.

```python
import math
import jax
import jax.numpy as jnp
from jax import lax

C = 64
H = 16
W = 16
MB = 4
SECTIONS = 4
DEPTH = 16
N_SECTION = 4


def level_of(rng, shape, split, least, largest):
    gain, own = 1.0, jax.random.fold_in(rng, 6)
    for dim, blocks in split:
        draws = jnp.exp(jax.random.uniform(jax.random.fold_in(own, dim), (blocks,), jnp.float32, least / len(split), largest / len(split)))
        gain = gain * jnp.repeat(draws, shape[dim] // blocks).reshape([-1 if axis == dim else 1 for axis in range(len(shape))])
    return gain


def gaussian(stream_key, dims, spread, bound, shards=(), dtype=jnp.bfloat16):
    loudness = level_of(stream_key, dims, shards, -0.22, 0.18) if shards else 1.0
    values = jax.random.normal(stream_key, dims, jnp.float32) * spread * loudness
    return jnp.minimum(jnp.maximum(values, -bound), bound).astype(dtype)


def setup_inputs(seed: int = 0) -> dict:
    streams_of = jax.random.split(jax.random.key(seed), 4)
    return {
        "activations": gaussian(streams_of[0], (SECTIONS, MB, DEPTH, C, H * W), 1.0, 6.0, ((0, 4), (2, 8)), jnp.float32),
        "filters": gaussian(streams_of[1], (SECTIONS, 27, C, C), (27 * C) ** -0.5, 0.15625, ((0, 4),), jnp.float32),
        "cotangent": gaussian(streams_of[2], (MB, DEPTH, C, H * W), 1.0, 6.0, ((1, 8),), jnp.float32),
    }


def convolve(volume, kernel_taps):
    depth_cells, channels, columns = volume.shape
    volume_grid = volume.reshape(1, depth_cells, channels, H, W).transpose(0, 2, 1, 3, 4)
    kernel = kernel_taps.reshape(3, 3, 3, channels, channels).transpose(3, 4, 0, 1, 2)
    result = lax.conv_general_dilated(volume_grid, kernel, (1, 1, 1), ((1, 1), (1, 1), (1, 1)), dimension_numbers=('NCDHW', 'OIDHW', 'NCDHW'), precision=lax.Precision.HIGHEST)
    return result[0].transpose(1, 0, 2, 3).reshape(depth_cells, channels, columns)

def silu_slope(preact):
    sigmoid_value = jax.nn.sigmoid(preact)
    return sigmoid_value * (1.0 + preact * (1.0 - sigmoid_value))

def reference(activations, filters, cotangent):
    upstream = [cotangent[micro_index] for micro_index in range(MB)]
    grad_layers = [None] * N_SECTION
    filter_layers = [None] * N_SECTION
    for layer_index in reversed(range(N_SECTION)):
        summed = jnp.zeros(filters.shape[1:], jnp.float32)
        outgoing = []
        for micro_index in range(MB):
            preact, pullback = jax.vjp(convolve, activations[layer_index, micro_index], filters[layer_index])
            slopes = upstream[micro_index] * silu_slope(preact)
            backward, filter_term = pullback(slopes)
            summed = summed + filter_term
            outgoing.append(backward)
        grad_layers[layer_index] = jnp.stack(outgoing)
        filter_layers[layer_index] = summed
        upstream = outgoing
    scaling = 1.0 / math.sqrt(MB * DEPTH * H * W)
    return (jnp.stack(grad_layers), jnp.stack(filter_layers) * scaling)
```

```python
import functools
import math

import jax
import jax.numpy as jnp
from jax import lax
from jax.experimental import pallas as pl
from jax.experimental.pallas import tpu as pltpu
from jax.sharding import PartitionSpec as P

H = 16
W = 16
F32 = jnp.float32
BF16 = jnp.bfloat16
MESH = pl.DeviceIdType.MESH


def split(x):
    hi = x.astype(BF16)
    return hi, (x - hi.astype(F32)).astype(BF16)


def tap_masks(cells):
    lane = lax.broadcasted_iota(jnp.int32, (1, cells), 1)
    y, x = lane // W, lane % W
    masks = []
    for b in (-1, 0, 1):
        for c in (-1, 0, 1):
            masks.append((y + b >= 0) & (y + b < H) & (x + c >= 0) & (x + c < W))
    return masks


def put_patches(plane, hi_ref, lo_ref, masks):
    ch, cells = plane.shape
    for k in range(9):
        by = (k // 3 - 1) * W + (k % 3 - 1)
        v = plane if by == 0 else pltpu.roll(plane, (-by) % cells, 1)
        if by != 0:
            v = jnp.where(masks[k], v, 0.0)
        hi, lo = split(v)
        hi_ref[k * ch : (k + 1) * ch, :] = hi
        lo_ref[k * ch : (k + 1) * ch, :] = lo


def dot(a, b):
    return jnp.dot(a, b, preferred_element_type=F32)


def dot_nt(a, b):
    return lax.dot_general(a, b, (((1,), (1,)), ((), ())), preferred_element_type=F32)


def kernel(
    n_sec, n_dep, scale,
    act, filt, cot,
    grads, fsum,
    ext, fbuf, up, slope, gbuf, fsend, frecv,
    p_hi, p_lo, s_hi, s_lo, fs, fh, gs, gh, ss, sh, acc,
    own_sem, filt_sem, cot_sem, halo_send, halo_recv, face_send, face_recv, hop_send, hop_recv, out_sem,
):
    mb, sp, ch, cells = act.shape
    sec, dep = lax.axis_index("section"), lax.axis_index("depth")
    is_last = sec == n_sec - 1
    has_prev, has_next = dep > 0, dep < n_dep - 1
    masks = tap_masks(cells)

    def own_copy(m):
        return pltpu.make_async_copy(act.at[m], ext.at[m, pl.ds(1, sp)], own_sem.at[m])

    filt_copy = pltpu.make_async_copy(filt, fbuf, filt_sem)
    filt_copy.start()
    for m in range(mb):
        own_copy(m).start()

    @pl.when(is_last)
    def _():
        for m in range(mb):
            pltpu.make_async_copy(cot.at[m], up.at[m], cot_sem.at[m]).start()

    barrier = pltpu.get_barrier_semaphore()
    for target in (
        (sec, (dep + 1) % n_dep), (sec, (dep + n_dep - 1) % n_dep),
        ((sec + 1) % n_sec, dep), ((sec + n_sec - 1) % n_sec, dep),
    ):
        pl.semaphore_signal(barrier, inc=1, device_id=target, device_id_type=MESH)
    pl.semaphore_wait(barrier, 4)

    def halo_to_prev(m):
        return pltpu.make_async_remote_copy(
            act.at[m, 0], ext.at[m, sp + 1], halo_send.at[0, m], halo_recv.at[0, m],
            device_id=(sec, dep - 1), device_id_type=MESH)

    def halo_to_next(m):
        return pltpu.make_async_remote_copy(
            act.at[m, sp - 1], ext.at[m, 0], halo_send.at[1, m], halo_recv.at[1, m],
            device_id=(sec, dep + 1), device_id_type=MESH)

    def face_to_prev(m):
        return pltpu.make_async_remote_copy(
            fsend.at[m, 0], frecv.at[m, 1], face_send.at[0, m], face_recv.at[0, m],
            device_id=(sec, dep - 1), device_id_type=MESH)

    def face_to_next(m):
        return pltpu.make_async_remote_copy(
            fsend.at[m, 1], frecv.at[m, 0], face_send.at[1, m], face_recv.at[1, m],
            device_id=(sec, dep + 1), device_id_type=MESH)

    def hop(m):
        return pltpu.make_async_remote_copy(
            gbuf.at[m], up.at[m], hop_send.at[m], hop_recv.at[m],
            device_id=(sec - 1, dep), device_id_type=MESH)

    def out_copy(m):
        return pltpu.make_async_copy(gbuf.at[m], grads.at[m], out_sem.at[m])

    @pl.when(has_prev)
    def _():
        for m in range(mb):
            halo_to_prev(m).start()

    @pl.when(has_next)
    def _():
        for m in range(mb):
            halo_to_next(m).start()

    @pl.when(jnp.logical_not(has_prev))
    def _():
        for m in range(mb):
            ext[m, 0] = jnp.zeros((ch, cells), F32)
            frecv[m, 0] = jnp.zeros((ch, cells), F32)

    @pl.when(jnp.logical_not(has_next))
    def _():
        for m in range(mb):
            ext[m, sp + 1] = jnp.zeros((ch, cells), F32)
            frecv[m, 1] = jnp.zeros((ch, cells), F32)

    filt_copy.wait()
    for k in range(27):
        a, k9 = k // 9, k % 9
        w = fbuf[k]
        hi, lo = split(w)
        cols = slice(k9 * ch, (k9 + 1) * ch)
        fs[2 * a * ch : (2 * a + 1) * ch, cols] = hi
        fs[(2 * a + 1) * ch : (2 * a + 2) * ch, cols] = lo
        fh[a * ch : (a + 1) * ch, cols] = hi
        hi, lo = split(w.T)
        cols = slice((8 - k9) * ch, (9 - k9) * ch)
        gs[2 * a * ch : (2 * a + 1) * ch, cols] = hi
        gs[(2 * a + 1) * ch : (2 * a + 2) * ch, cols] = lo
        gh[a * ch : (a + 1) * ch, cols] = hi
    acc[...] = jnp.zeros_like(acc)

    def taps_of(e):
        return max(0, e - (sp - 1)), min(2, e)

    def prep(m):
        own_copy(m).wait()
        pre = [None] * sp
        for e in [*range(1, sp + 1), 0, sp + 1]:
            if e == 0:
                @pl.when(has_next)
                def _():
                    halo_to_prev(m).wait_recv()

                @pl.when(has_prev)
                def _():
                    halo_to_next(m).wait_recv()
            hi_ref, lo_ref = p_hi.at[m, e], p_lo.at[m, e]
            put_patches(ext[m, e], hi_ref, lo_ref, masks)
            a0, a1 = taps_of(e)
            yh = dot(fs[2 * a0 * ch : 2 * (a1 + 1) * ch, :], hi_ref[...])
            yl = dot(fh[a0 * ch : (a1 + 1) * ch, :], lo_ref[...])
            for a in range(a0, a1 + 1):
                j = a - a0
                part = (yh[2 * j * ch : (2 * j + 1) * ch] + yh[(2 * j + 1) * ch : (2 * j + 2) * ch]
                        + yl[j * ch : (j + 1) * ch])
                d = e - a
                pre[d] = part if pre[d] is None else pre[d] + part
        for d in range(sp):
            sg = jax.nn.sigmoid(pre[d])
            slope[m, d] = sg * (1.0 + pre[d] * (1.0 - sg))

    def back(d, a0, a1):
        yh = dot(gs[2 * a0 * ch : 2 * (a1 + 1) * ch, :], s_hi[d])
        yl = dot(gh[a0 * ch : (a1 + 1) * ch, :], s_lo[d])
        return [
            yh[2 * j * ch : (2 * j + 1) * ch] + yh[(2 * j + 1) * ch : (2 * j + 2) * ch] + yl[j * ch : (j + 1) * ch]
            for j in range(a1 - a0 + 1)
        ]

    prep(0)

    @pl.when(jnp.logical_not(is_last))
    def _():
        def more(m, carry):
            prep(m)
            return carry
        lax.fori_loop(1, mb, more, 0)

    def step(m, carry):
        @pl.when(is_last)
        def _():
            pltpu.make_async_copy(cot.at[m], up.at[m], cot_sem.at[m]).wait()

        @pl.when(jnp.logical_not(is_last))
        def _():
            hop(m).wait_recv()

        for d in range(sp):
            s = up[m, d] * slope[m, d]
            hi, lo = split(s)
            r = sp - 1 - d
            ss[2 * r * ch : (2 * r + 1) * ch, :] = hi
            ss[(2 * r + 1) * ch : (2 * r + 2) * ch, :] = lo
            sh[r * ch : (r + 1) * ch, :] = hi
            put_patches(s, s_hi.at[d], s_lo.at[d], masks)
        fsend[m, 0] = back(0, 0, 0)[0]

        @pl.when(has_prev)
        def _():
            face_to_prev(m).start()

        fsend[m, 1] = back(sp - 1, 2, 2)[0]

        @pl.when(has_next)
        def _():
            face_to_next(m).start()

        out = [None] * sp
        for d in range(sp):
            a0 = 1 if d == 0 else 0
            a1 = 1 if d == sp - 1 else 2
            for j, part in enumerate(back(d, a0, a1)):
                o = d + a0 + j - 1
                out[o] = part if out[o] is None else out[o] + part
        for d in range(sp):
            gbuf[m, d] = out[d]

        @pl.when(is_last & (m + 1 < mb))
        def _():
            prep(jnp.minimum(m + 1, mb - 1))

        @pl.when(has_next)
        def _():
            face_to_prev(m).wait_recv()

        @pl.when(has_prev)
        def _():
            face_to_next(m).wait_recv()

        gbuf[m, 0] = gbuf[m, 0] + frecv[m, 0]
        gbuf[m, sp - 1] = gbuf[m, sp - 1] + frecv[m, 1]

        @pl.when(sec > 0)
        def _():
            hop(m).start()

        out_copy(m).start()

        for e in range(sp + 2):
            a0, a1 = taps_of(e)
            r0 = sp - 1 - (e - a0)
            n = a1 - a0 + 1
            yh = dot_nt(ss[2 * r0 * ch : 2 * (r0 + n) * ch, :], p_hi[m, e])
            yl = dot_nt(sh[r0 * ch : (r0 + n) * ch, :], p_lo[m, e])
            for j in range(n):
                a = a0 + j
                acc[a * ch : (a + 1) * ch, :] += (
                    yh[2 * j * ch : (2 * j + 1) * ch] + yh[(2 * j + 1) * ch : (2 * j + 2) * ch]
                    + yl[j * ch : (j + 1) * ch])
        return carry

    lax.fori_loop(0, mb, step, 0)
    fsum[...] = acc[...] * scale

    for m in range(mb):
        out_copy(m).wait()

    @pl.when(has_prev)
    def _():
        for m in range(mb):
            halo_to_prev(m).wait_send()
            face_to_prev(m).wait_send()

    @pl.when(has_next)
    def _():
        for m in range(mb):
            halo_to_next(m).wait_send()
            face_to_next(m).wait_send()

    @pl.when(sec > 0)
    def _():
        for m in range(mb):
            hop(m).wait_send()


def per_device(n_sec, n_dep, activations, filters, cotangent):
    act, filt = activations[0], filters[0]
    mb, sp, ch, cells = act.shape
    scale = 1.0 / math.sqrt(mb * sp * n_dep * H * W)
    any_spec = pl.BlockSpec(memory_space=pl.ANY)
    dma = pltpu.SemaphoreType.DMA
    grads, fsum = pl.pallas_call(
        functools.partial(kernel, n_sec, n_dep, scale),
        out_shape=(
            jax.ShapeDtypeStruct(act.shape, F32),
            jax.ShapeDtypeStruct((3 * ch, 9 * ch), F32),
        ),
        in_specs=[any_spec] * 3,
        out_specs=(any_spec, pl.BlockSpec(memory_space=pltpu.VMEM)),
        scratch_shapes=[
            pltpu.VMEM((mb, sp + 2, ch, cells), F32),
            pltpu.VMEM(filt.shape, F32),
            pltpu.VMEM((mb, sp, ch, cells), F32),
            pltpu.VMEM((mb, sp, ch, cells), F32),
            pltpu.VMEM((mb, sp, ch, cells), F32),
            pltpu.VMEM((mb, 2, ch, cells), F32),
            pltpu.VMEM((mb, 2, ch, cells), F32),
            pltpu.VMEM((mb, sp + 2, 9 * ch, cells), BF16),
            pltpu.VMEM((mb, sp + 2, 9 * ch, cells), BF16),
            pltpu.VMEM((sp, 9 * ch, cells), BF16),
            pltpu.VMEM((sp, 9 * ch, cells), BF16),
            pltpu.VMEM((6 * ch, 9 * ch), BF16),
            pltpu.VMEM((3 * ch, 9 * ch), BF16),
            pltpu.VMEM((6 * ch, 9 * ch), BF16),
            pltpu.VMEM((3 * ch, 9 * ch), BF16),
            pltpu.VMEM((2 * sp * ch, cells), BF16),
            pltpu.VMEM((sp * ch, cells), BF16),
            pltpu.VMEM((3 * ch, 9 * ch), F32),
            dma((mb,)), dma, dma((mb,)),
            dma((2, mb)), dma((2, mb)), dma((2, mb)), dma((2, mb)),
            dma((mb,)), dma((mb,)), dma((mb,)),
        ],
        compiler_params=pltpu.CompilerParams(
            collective_id=0, has_side_effects=True, vmem_limit_bytes=48 * 1024 * 1024),
    )(act, filt, cotangent)
    summed = lax.psum(fsum, "depth")
    summed = summed.reshape(3, ch, 9, ch).transpose(0, 2, 1, 3).reshape(27, ch, ch)
    return grads[None], summed[None]


def solution(mesh):
    return jax.shard_map(
        functools.partial(per_device, mesh.shape["section"], mesh.shape["depth"]),
        mesh=mesh,
        in_specs=(
            P("section", None, "depth", None, None),
            P("section", None, None, None),
            P(None, "depth", None, None),
        ),
        out_specs=(P("section", None, "depth", None, None), P("section", None, None, None)),
        check_vma=False,
    )
```

```python
import functools
import math

import jax
import jax.numpy as jnp
from jax import lax
from jax.experimental import pallas as pl
from jax.experimental.pallas import tpu as pltpu
from jax.sharding import PartitionSpec as P

H = 16
W = 16
F32 = jnp.float32
BF16 = jnp.bfloat16
MESH = pl.DeviceIdType.MESH


def split(x):
    hi = x.astype(BF16)
    return hi, (x - hi.astype(F32)).astype(BF16)


def tap_masks(cells):
    lane = lax.broadcasted_iota(jnp.int32, (1, cells), 1)
    y, x = lane // W, lane % W
    masks = []
    for b in (-1, 0, 1):
        for c in (-1, 0, 1):
            masks.append((y + b >= 0) & (y + b < H) & (x + c >= 0) & (x + c < W))
    return masks


def put_patches(plane, hi_ref, lo_ref, masks):
    ch, cells = plane.shape
    for k in range(9):
        by = (k // 3 - 1) * W + (k % 3 - 1)
        v = plane if by == 0 else pltpu.roll(plane, (-by) % cells, 1)
        if by != 0:
            v = jnp.where(masks[k], v, 0.0)
        hi, lo = split(v)
        hi_ref[k * ch : (k + 1) * ch, :] = hi
        lo_ref[k * ch : (k + 1) * ch, :] = lo


def dot(a, b):
    return jnp.dot(a, b, preferred_element_type=F32)


def dot_nt(a, b):
    return lax.dot_general(a, b, (((1,), (1,)), ((), ())), preferred_element_type=F32)


def kernel(
    n_sec, n_dep, scale,
    act, filt, cot,
    grads, fsum,
    ext, fbuf, up, slope, gbuf, fsend, frecv,
    p_hi, p_lo, s_hi, s_lo, fs, fh, gs, gh, ss, sh, acc,
    pbuf, hbuf, cbuf, full,
    own_sem, filt_sem, cot_sem, halo_send, halo_recv, face_send, face_recv, hop_send, hop_recv, out_sem,
    pair_send, pair_recv, rs_send, rs_recv, ag_send, ag_recv, fw_send, fw_recv, fout_sem,
):
    mb, sp, ch, cells = act.shape
    sec, dep = lax.axis_index("section"), lax.axis_index("depth")
    is_last = sec == n_sec - 1
    has_prev, has_next = dep > 0, dep < n_dep - 1
    masks = tap_masks(cells)

    def own_copy(m):
        return pltpu.make_async_copy(act.at[m], ext.at[m, pl.ds(1, sp)], own_sem.at[m])

    filt_copy = pltpu.make_async_copy(filt, fbuf, filt_sem)
    filt_copy.start()
    for m in range(mb):
        own_copy(m).start()

    @pl.when(is_last)
    def _():
        for m in range(mb):
            pltpu.make_async_copy(cot.at[m], up.at[m], cot_sem.at[m]).start()

    n2 = n_dep // 2
    half = acc.shape[0] // 2
    rs = half // n2
    zed, core = dep // 2, dep % 2
    partner = (sec, zed * 2 + 1 - core)

    def peer(t):
        return (sec, ((zed + t) % n2) * 2 + core)

    barrier = pltpu.get_barrier_semaphore()
    for t in range(1, n2):
        pl.semaphore_signal(barrier, inc=1, device_id=peer(t), device_id_type=MESH)
    for target in (
        (sec, (dep + 1) % n_dep), (sec, (dep + n_dep - 1) % n_dep),
        ((sec + 1) % n_sec, dep), ((sec + n_sec - 1) % n_sec, dep),
    ):
        pl.semaphore_signal(barrier, inc=1, device_id=target, device_id_type=MESH)
    pl.semaphore_wait(barrier, 3 + n2)

    def halo_to_prev(m):
        return pltpu.make_async_remote_copy(
            act.at[m, 0], ext.at[m, sp + 1], halo_send.at[0, m], halo_recv.at[0, m],
            device_id=(sec, dep - 1), device_id_type=MESH)

    def halo_to_next(m):
        return pltpu.make_async_remote_copy(
            act.at[m, sp - 1], ext.at[m, 0], halo_send.at[1, m], halo_recv.at[1, m],
            device_id=(sec, dep + 1), device_id_type=MESH)

    def face_to_prev(m):
        return pltpu.make_async_remote_copy(
            fsend.at[m, 0], frecv.at[m, 1], face_send.at[0, m], face_recv.at[0, m],
            device_id=(sec, dep - 1), device_id_type=MESH)

    def face_to_next(m):
        return pltpu.make_async_remote_copy(
            fsend.at[m, 1], frecv.at[m, 0], face_send.at[1, m], face_recv.at[1, m],
            device_id=(sec, dep + 1), device_id_type=MESH)

    def hop(m):
        return pltpu.make_async_remote_copy(
            gbuf.at[m], up.at[m], hop_send.at[m], hop_recv.at[m],
            device_id=(sec - 1, dep), device_id_type=MESH)

    def out_copy(m):
        return pltpu.make_async_copy(gbuf.at[m], grads.at[m], out_sem.at[m])

    def remote(src, dst, send, recv, target):
        return pltpu.make_async_remote_copy(src, dst, send, recv, device_id=target, device_id_type=MESH)

    def pair():
        theirs = pl.multiple_of((1 - core) * half, 8)
        return remote(acc.at[pl.ds(theirs, half)], pbuf, pair_send, pair_recv, partner)

    def scatter(t):
        rows = pl.ds(pl.multiple_of(((zed + t) % n2) * rs, 8), rs)
        return remote(hbuf.at[rows], cbuf.at[t - 1], rs_send.at[t - 1], rs_recv.at[t - 1], peer(t))

    def rows_of(t):
        return pl.ds(pl.multiple_of(core * half + ((zed + n2 - t) % n2) * rs, 8), rs)

    def gather(t):
        return remote(full.at[rows_of(0)], full.at[rows_of(0)], ag_send.at[t - 1], ag_recv.at[t - 1], peer(t))

    def arrived(t):
        return remote(full.at[rows_of(t)], full.at[rows_of(t)], ag_send.at[t - 1], ag_recv.at[t - 1], peer(t))

    def forward(t):
        return remote(full.at[rows_of(t)], full.at[rows_of(t)], fw_send.at[t], fw_recv.at[t], partner)

    @pl.when(has_prev)
    def _():
        for m in range(mb):
            halo_to_prev(m).start()

    @pl.when(has_next)
    def _():
        for m in range(mb):
            halo_to_next(m).start()

    @pl.when(jnp.logical_not(has_prev))
    def _():
        for m in range(mb):
            ext[m, 0] = jnp.zeros((ch, cells), F32)
            frecv[m, 0] = jnp.zeros((ch, cells), F32)

    @pl.when(jnp.logical_not(has_next))
    def _():
        for m in range(mb):
            ext[m, sp + 1] = jnp.zeros((ch, cells), F32)
            frecv[m, 1] = jnp.zeros((ch, cells), F32)

    filt_copy.wait()
    for k in range(27):
        a, k9 = k // 9, k % 9
        w = fbuf[k]
        hi, lo = split(w)
        cols = slice(k9 * ch, (k9 + 1) * ch)
        fs[2 * a * ch : (2 * a + 1) * ch, cols] = hi
        fs[(2 * a + 1) * ch : (2 * a + 2) * ch, cols] = lo
        fh[a * ch : (a + 1) * ch, cols] = hi
        hi, lo = split(w.T)
        cols = slice((8 - k9) * ch, (9 - k9) * ch)
        gs[2 * a * ch : (2 * a + 1) * ch, cols] = hi
        gs[(2 * a + 1) * ch : (2 * a + 2) * ch, cols] = lo
        gh[a * ch : (a + 1) * ch, cols] = hi
    acc[...] = jnp.zeros_like(acc)

    def taps_of(e):
        return max(0, e - (sp - 1)), min(2, e)

    def prep(m):
        own_copy(m).wait()
        pre = [None] * sp
        for e in [*range(1, sp + 1), 0, sp + 1]:
            if e == 0:
                @pl.when(has_next)
                def _():
                    halo_to_prev(m).wait_recv()

                @pl.when(has_prev)
                def _():
                    halo_to_next(m).wait_recv()
            hi_ref, lo_ref = p_hi.at[m, e], p_lo.at[m, e]
            put_patches(ext[m, e], hi_ref, lo_ref, masks)
            a0, a1 = taps_of(e)
            yh = dot(fs[2 * a0 * ch : 2 * (a1 + 1) * ch, :], hi_ref[...])
            yl = dot(fh[a0 * ch : (a1 + 1) * ch, :], lo_ref[...])
            for a in range(a0, a1 + 1):
                j = a - a0
                part = (yh[2 * j * ch : (2 * j + 1) * ch] + yh[(2 * j + 1) * ch : (2 * j + 2) * ch]
                        + yl[j * ch : (j + 1) * ch])
                d = e - a
                pre[d] = part if pre[d] is None else pre[d] + part
        for d in range(sp):
            sg = jax.nn.sigmoid(pre[d])
            slope[m, d] = sg * (1.0 + pre[d] * (1.0 - sg))

    def back(d, a0, a1):
        yh = dot(gs[2 * a0 * ch : 2 * (a1 + 1) * ch, :], s_hi[d])
        yl = dot(gh[a0 * ch : (a1 + 1) * ch, :], s_lo[d])
        return [
            yh[2 * j * ch : (2 * j + 1) * ch] + yh[(2 * j + 1) * ch : (2 * j + 2) * ch] + yl[j * ch : (j + 1) * ch]
            for j in range(a1 - a0 + 1)
        ]

    def filter_terms(m):
        for e in range(sp + 2):
            a0, a1 = taps_of(e)
            r0 = sp - 1 - (e - a0)
            n = a1 - a0 + 1
            yh = dot_nt(ss[2 * r0 * ch : 2 * (r0 + n) * ch, :], p_hi[m, e])
            yl = dot_nt(sh[r0 * ch : (r0 + n) * ch, :], p_lo[m, e])
            for j in range(n):
                a = a0 + j
                acc[a * ch : (a + 1) * ch, :] += (
                    yh[2 * j * ch : (2 * j + 1) * ch] + yh[(2 * j + 1) * ch : (2 * j + 2) * ch]
                    + yl[j * ch : (j + 1) * ch])

    prep(0)

    @pl.when(jnp.logical_not(is_last))
    def _():
        def more(m, carry):
            prep(m)
            return carry
        lax.fori_loop(1, mb, more, 0)

    def step(m, carry):
        @pl.when(is_last)
        def _():
            pltpu.make_async_copy(cot.at[m], up.at[m], cot_sem.at[m]).wait()

        @pl.when(jnp.logical_not(is_last))
        def _():
            hop(m).wait_recv()

        def cotangents(d):
            s = up[m, d] * slope[m, d]
            hi, lo = split(s)
            r = sp - 1 - d
            ss[2 * r * ch : (2 * r + 1) * ch, :] = hi
            ss[(2 * r + 1) * ch : (2 * r + 2) * ch, :] = lo
            sh[r * ch : (r + 1) * ch, :] = hi
            put_patches(s, s_hi.at[d], s_lo.at[d], masks)

        cotangents(0)
        fsend[m, 0] = back(0, 0, 0)[0]

        @pl.when(has_prev)
        def _():
            face_to_prev(m).start()

        for d in range(1, sp):
            cotangents(d)
        fsend[m, 1] = back(sp - 1, 2, 2)[0]

        @pl.when(has_next)
        def _():
            face_to_next(m).start()

        @pl.when(sec == 0)
        def _():
            filter_terms(m)

        @pl.when((sec == 0) & (m == mb - 1))
        def _():
            pair().start()

        out = [None] * sp
        for d in range(sp):
            a0 = 1 if d == 0 else 0
            a1 = 1 if d == sp - 1 else 2
            for j, part in enumerate(back(d, a0, a1)):
                o = d + a0 + j - 1
                out[o] = part if out[o] is None else out[o] + part
        for d in range(sp):
            gbuf[m, d] = out[d]

        @pl.when(is_last & (m + 1 < mb))
        def _():
            prep(jnp.minimum(m + 1, mb - 1))

        @pl.when(has_next)
        def _():
            face_to_prev(m).wait_recv()

        @pl.when(has_prev)
        def _():
            face_to_next(m).wait_recv()

        gbuf[m, 0] = gbuf[m, 0] + frecv[m, 0]
        gbuf[m, sp - 1] = gbuf[m, sp - 1] + frecv[m, 1]

        @pl.when(sec > 0)
        def _():
            hop(m).start()

        out_copy(m).start()

        @pl.when(sec > 0)
        def _():
            filter_terms(m)

        return carry

    lax.fori_loop(0, mb, step, 0)

    @pl.when(sec > 0)
    def _():
        pair().start()

    mine = pl.multiple_of(core * half, 8)
    pair().wait_recv()
    hbuf[...] = acc[pl.ds(mine, half), :] + pbuf[...]
    for t in range(1, n2):
        scatter(t).start()
    total = hbuf[pl.ds(pl.multiple_of(zed * rs, 8), rs), :]
    for t in range(1, n2):
        scatter(t).wait_recv()
        total = total + cbuf[t - 1]
    full[rows_of(0), :] = total * scale
    for t in range(1, n2):
        gather(t).start()
    forward(0).start()
    for t in range(1, n2):
        arrived(t).wait_recv()
        forward(t).start()
    for t in range(n2):
        forward(t).wait_recv()
    for k in range(27):
        a, k9 = k // 9, k % 9
        fbuf[k] = full[a * ch : (a + 1) * ch, k9 * ch : (k9 + 1) * ch]
    fout = pltpu.make_async_copy(fbuf, fsum, fout_sem)
    fout.start()
    pair().wait_send()
    for t in range(1, n2):
        scatter(t).wait_send()
        gather(t).wait_send()
    for t in range(n2):
        forward(t).wait_send()
    fout.wait()

    for m in range(mb):
        out_copy(m).wait()

    @pl.when(has_prev)
    def _():
        for m in range(mb):
            halo_to_prev(m).wait_send()
            face_to_prev(m).wait_send()

    @pl.when(has_next)
    def _():
        for m in range(mb):
            halo_to_next(m).wait_send()
            face_to_next(m).wait_send()

    @pl.when(sec > 0)
    def _():
        for m in range(mb):
            hop(m).wait_send()


def per_device(n_sec, n_dep, activations, filters, cotangent):
    act, filt = activations[0], filters[0]
    mb, sp, ch, cells = act.shape
    scale = 1.0 / math.sqrt(mb * sp * n_dep * H * W)
    any_spec = pl.BlockSpec(memory_space=pl.ANY)
    hbm_spec = pl.BlockSpec(memory_space=pltpu.MemorySpace.HBM)
    n2 = n_dep // 2
    rs = 8 * pl.cdiv(3 * ch, 16 * n2)
    dma = pltpu.SemaphoreType.DMA
    grads, fsum = pl.pallas_call(
        functools.partial(kernel, n_sec, n_dep, scale),
        out_shape=(
            jax.ShapeDtypeStruct(act.shape, F32),
            jax.ShapeDtypeStruct(filt.shape, F32),
        ),
        in_specs=[hbm_spec] * 3,
        out_specs=(any_spec, any_spec),
        scratch_shapes=[
            pltpu.VMEM((mb, sp + 2, ch, cells), F32),
            pltpu.VMEM(filt.shape, F32),
            pltpu.VMEM((mb, sp, ch, cells), F32),
            pltpu.VMEM((mb, sp, ch, cells), F32),
            pltpu.VMEM((mb, sp, ch, cells), F32),
            pltpu.VMEM((mb, 2, ch, cells), F32),
            pltpu.VMEM((mb, 2, ch, cells), F32),
            pltpu.VMEM((mb, sp + 2, 9 * ch, cells), BF16),
            pltpu.VMEM((mb, sp + 2, 9 * ch, cells), BF16),
            pltpu.VMEM((sp, 9 * ch, cells), BF16),
            pltpu.VMEM((sp, 9 * ch, cells), BF16),
            pltpu.VMEM((6 * ch, 9 * ch), BF16),
            pltpu.VMEM((3 * ch, 9 * ch), BF16),
            pltpu.VMEM((6 * ch, 9 * ch), BF16),
            pltpu.VMEM((3 * ch, 9 * ch), BF16),
            pltpu.VMEM((2 * sp * ch, cells), BF16),
            pltpu.VMEM((sp * ch, cells), BF16),
            pltpu.VMEM((2 * n2 * rs, 9 * ch), F32),
            pltpu.VMEM((n2 * rs, 9 * ch), F32),
            pltpu.VMEM((n2 * rs, 9 * ch), F32),
            pltpu.VMEM((max(n2 - 1, 1), rs, 9 * ch), F32),
            pltpu.VMEM((2 * n2 * rs, 9 * ch), F32),
            dma((mb,)), dma, dma((mb,)),
            dma((2, mb)), dma((2, mb)), dma((2, mb)), dma((2, mb)),
            dma((mb,)), dma((mb,)), dma((mb,)),
            dma, dma, dma((n2,)), dma((n2,)), dma((n2,)), dma((n2,)), dma((n2,)), dma((n2,)), dma,
        ],
        compiler_params=pltpu.CompilerParams(
            collective_id=0, has_side_effects=True, vmem_limit_bytes=48 * 1024 * 1024),
    )(act, filt, cotangent)
    return grads[None], fsum[None]


def solution(mesh):
    return jax.shard_map(
        functools.partial(per_device, mesh.shape["section"], mesh.shape["depth"]),
        mesh=mesh,
        in_specs=(
            P("section", None, "depth", None, None),
            P("section", None, None, None),
            P(None, "depth", None, None),
        ),
        out_specs=(P("section", None, "depth", None, None), P("section", None, None, None)),
        check_vma=False,
    )
```

```python
import functools
import math

import jax
import jax.numpy as jnp
from jax import lax
from jax.experimental import pallas as pl
from jax.experimental.pallas import tpu as pltpu
from jax.sharding import PartitionSpec as P

H = 16
W = 16
F32 = jnp.float32
BF16 = jnp.bfloat16
MESH = pl.DeviceIdType.MESH


def split(x):
    hi = x.astype(BF16)
    return hi, (x - hi.astype(F32)).astype(BF16)


def tap_masks(cells):
    lane = lax.broadcasted_iota(jnp.int32, (1, cells), 1)
    y, x = lane // W, lane % W
    masks = []
    for b in (-1, 0, 1):
        for c in (-1, 0, 1):
            masks.append((y + b >= 0) & (y + b < H) & (x + c >= 0) & (x + c < W))
    return masks


def put_patches(plane, hi_ref, lo_ref, masks):
    ch, cells = plane.shape
    for k in range(9):
        by = (k // 3 - 1) * W + (k % 3 - 1)
        v = plane if by == 0 else pltpu.roll(plane, (-by) % cells, 1)
        if by != 0:
            v = jnp.where(masks[k], v, 0.0)
        hi, lo = split(v)
        hi_ref[k * ch : (k + 1) * ch, :] = hi
        lo_ref[k * ch : (k + 1) * ch, :] = lo


def dot(a, b):
    return jnp.dot(a, b, preferred_element_type=F32)


def dot_nt(a, b):
    return lax.dot_general(a, b, (((1,), (1,)), ((), ())), preferred_element_type=F32)


def kernel(
    n_sec, n_dep, scale,
    act, filt, cot,
    grads, fsum,
    ext, fbuf, up, slope, gbuf, fsend, frecv,
    p_hi, p_lo, s_hi, s_lo, fs, fh, gs, gh, ss, sh, acc,
    pbuf, hbuf, cbuf, full,
    own_sem, filt_sem, cot_sem, halo_send, halo_recv, face_send, face_recv, hop_send, hop_recv, out_sem,
    pair_send, pair_recv, rs_send, rs_recv, ag_send, ag_recv, fw_send, fw_recv, fout_sem,
):
    mb, sp, ch, cells = act.shape
    sec, dep = lax.axis_index("section"), lax.axis_index("depth")
    n2 = n_dep // 2
    zed, core = dep // 2, dep % 2
    is_last = sec == n_sec - 1
    toward = 2 * core - 1
    outer_dep = dep + toward
    has_outer = (outer_dep >= 0) & (outer_dep < n_dep)
    partner, outside = (sec, dep - toward), (sec, outer_dep)
    masks = tap_masks(cells)

    def plane(j):
        return core * j + (1 - core) * (sp - 1 - j)

    def tap(a):
        return core * a + (1 - core) * (2 - a)

    def remote(src, dst, send, recv, target):
        return pltpu.make_async_remote_copy(src, dst, send, recv, device_id=target, device_id_type=MESH)

    def own_copy(m, j):
        return pltpu.make_async_copy(act.at[m, plane(j)], ext.at[m, j + 1], own_sem.at[m, j])

    def cot_copy(m, j):
        return pltpu.make_async_copy(cot.at[m, plane(j)], up.at[m, j], cot_sem.at[m, j])

    filt_copy = pltpu.make_async_copy(filt, fbuf, filt_sem)
    filt_copy.start()
    for m in range(mb):
        for j in range(sp):
            own_copy(m, j).start()

    @pl.when(is_last)
    def _():
        for m in range(mb):
            for j in range(sp):
                cot_copy(m, j).start()

    half = acc.shape[0] // 2
    rs = half // n2
    pieces = rs // 8

    def peer(t):
        return (sec, ((zed + t) % n2) * 2 + core)

    barrier = pltpu.get_barrier_semaphore()
    for target in (
        (sec, (dep + 1) % n_dep), (sec, (dep + n_dep - 1) % n_dep),
        ((sec + 1) % n_sec, dep), ((sec + n_sec - 1) % n_sec, dep),
        *(peer(t) for t in range(1, n2)),
    ):
        pl.semaphore_signal(barrier, inc=1, device_id=target, device_id_type=MESH)
    pl.semaphore_wait(barrier, 3 + n2)

    def halo_in(m):
        return remote(act.at[m, plane(0)], ext.at[m, 0], halo_send.at[0, m], halo_recv.at[0, m], partner)

    def halo_out(m):
        return remote(act.at[m, plane(sp - 1)], ext.at[m, sp + 1], halo_send.at[1, m], halo_recv.at[1, m], outside)

    def face_in(m):
        return remote(fsend.at[m, 0], frecv.at[m, 0], face_send.at[0, m], face_recv.at[0, m], partner)

    def face_out(m):
        return remote(fsend.at[m, 1], frecv.at[m, 1], face_send.at[1, m], face_recv.at[1, m], outside)

    def hop(m, j):
        return remote(gbuf.at[m, j], up.at[m, j], hop_send.at[m, j], hop_recv.at[m, j], (sec - 1, dep))

    def out_copy(m, j):
        return pltpu.make_async_copy(gbuf.at[m, j], grads.at[m, plane(j)], out_sem.at[m, j])

    def pair():
        theirs = pl.multiple_of((1 - core) * half, 8)
        return remote(acc.at[pl.ds(theirs, half)], pbuf, pair_send, pair_recv, partner)

    def scatter(p, t):
        rows = pl.ds(pl.multiple_of(((zed + t) % n2) * rs + p * 8, 8), 8)
        return remote(hbuf.at[rows], cbuf.at[t - 1, pl.ds(p * 8, 8)], rs_send.at[p, t - 1], rs_recv.at[p, t - 1], peer(t))

    def rows_of(p, t):
        return pl.ds(pl.multiple_of(core * half + ((zed + n2 - t) % n2) * rs + p * 8, 8), 8)

    def gather(p, t):
        rows = rows_of(p, 0)
        return remote(full.at[rows], full.at[rows], ag_send.at[p, t - 1], ag_recv.at[p, t - 1], peer(t))

    def arrived(p, t):
        rows = rows_of(p, t)
        return remote(full.at[rows], full.at[rows], ag_send.at[p, t - 1], ag_recv.at[p, t - 1], peer(t))

    def forward(p, t):
        rows = rows_of(p, t)
        return remote(full.at[rows], full.at[rows], fw_send.at[p, t], fw_recv.at[p, t], partner)

    for m in range(mb):
        halo_in(m).start()

    @pl.when(has_outer)
    def _():
        for m in range(mb):
            halo_out(m).start()

    @pl.when(jnp.logical_not(has_outer))
    def _():
        for m in range(mb):
            ext[m, sp + 1] = jnp.zeros((ch, cells), F32)
            frecv[m, 1] = jnp.zeros((ch, cells), F32)

    filt_copy.wait()
    for a in range(3):
        r = tap(a)
        two, one = pl.multiple_of(2 * r * ch, 2 * ch), pl.multiple_of(r * ch, ch)
        for k9 in range(9):
            w = fbuf[9 * a + k9]
            hi, lo = split(w)
            cols = slice(k9 * ch, (k9 + 1) * ch)
            fs[pl.ds(two, ch), cols] = hi
            fs[pl.ds(two + ch, ch), cols] = lo
            fh[pl.ds(one, ch), cols] = hi
            hi, lo = split(w.T)
            cols = slice((8 - k9) * ch, (9 - k9) * ch)
            gs[pl.ds(two, ch), cols] = hi
            gs[pl.ds(two + ch, ch), cols] = lo
            gh[pl.ds(one, ch), cols] = hi
    acc[...] = jnp.zeros_like(acc)

    def taps_of(e):
        return max(0, e - (sp - 1)), min(2, e)

    def parts(yh, yl, n):
        return [
            yh[2 * i * ch : (2 * i + 1) * ch] + yh[(2 * i + 1) * ch : (2 * i + 2) * ch] + yl[i * ch : (i + 1) * ch]
            for i in range(n)
        ]

    def prep(m):
        pre = [None] * sp
        for e in [*range(1, sp + 1), 0, sp + 1]:
            if e == 0:
                halo_in(m).wait_recv()
            elif e <= sp:
                own_copy(m, e - 1).wait()
            else:
                @pl.when(has_outer)
                def _():
                    halo_out(m).wait_recv()
            hi_ref, lo_ref = p_hi.at[m, e], p_lo.at[m, e]
            put_patches(ext[m, e], hi_ref, lo_ref, masks)
            a0, a1 = taps_of(e)
            yh = dot(fs[2 * a0 * ch : 2 * (a1 + 1) * ch, :], hi_ref[...])
            yl = dot(fh[a0 * ch : (a1 + 1) * ch, :], lo_ref[...])
            for i, part in enumerate(parts(yh, yl, a1 - a0 + 1)):
                d = e - a0 - i
                pre[d] = part if pre[d] is None else pre[d] + part
        for d in range(sp):
            sg = jax.nn.sigmoid(pre[d])
            slope[m, d] = sg * (1.0 + pre[d] * (1.0 - sg))

    def back(d, a0, a1):
        yh = dot(gs[2 * a0 * ch : 2 * (a1 + 1) * ch, :], s_hi[d])
        yl = dot(gh[a0 * ch : (a1 + 1) * ch, :], s_lo[d])
        return parts(yh, yl, a1 - a0 + 1)

    def filter_terms(m):
        for e in range(sp + 2):
            a0, a1 = taps_of(e)
            r0 = sp - 1 - (e - a0)
            n = a1 - a0 + 1
            yh = dot_nt(ss[2 * r0 * ch : 2 * (r0 + n) * ch, :], p_hi[m, e])
            yl = dot_nt(sh[r0 * ch : (r0 + n) * ch, :], p_lo[m, e])
            for i, part in enumerate(parts(yh, yl, n)):
                rows = pl.ds(pl.multiple_of(tap(a0 + i) * ch, ch), ch)
                acc[rows, :] += part

    prep(0)

    @pl.when(jnp.logical_not(is_last))
    def _():
        def more(m, carry):
            prep(m)
            return carry
        lax.fori_loop(1, mb, more, 0)

    def step(m, carry):
        def cotangents(d):
            @pl.when(is_last)
            def _():
                cot_copy(m, d).wait()

            @pl.when(jnp.logical_not(is_last))
            def _():
                hop(m, d).wait_recv()

            s = up[m, d] * slope[m, d]
            hi, lo = split(s)
            r = sp - 1 - d
            ss[2 * r * ch : (2 * r + 1) * ch, :] = hi
            ss[(2 * r + 1) * ch : (2 * r + 2) * ch, :] = lo
            sh[r * ch : (r + 1) * ch, :] = hi
            put_patches(s, s_hi.at[d], s_lo.at[d], masks)

        def leave(j):
            @pl.when(sec > 0)
            def _():
                hop(m, j).start()

            out_copy(m, j).start()

        cotangents(0)
        fsend[m, 0] = back(0, 0, 0)[0]
        face_in(m).start()
        for d in range(1, sp):
            cotangents(d)
        fsend[m, 1] = back(sp - 1, 2, 2)[0]

        @pl.when(has_outer)
        def _():
            face_out(m).start()

        @pl.when(sec == 0)
        def _():
            filter_terms(m)

        @pl.when((sec == 0) & (m == mb - 1))
        def _():
            pair().start()

        out = [None] * sp
        for d in range(sp):
            a0 = 1 if d == 0 else 0
            a1 = 1 if d == sp - 1 else 2
            for i, part in enumerate(back(d, a0, a1)):
                o = d + a0 + i - 1
                out[o] = part if out[o] is None else out[o] + part
        for d in range(1, sp):
            gbuf[m, d] = out[d]
        face_in(m).wait_recv()
        gbuf[m, 0] = out[0] + frecv[m, 0]
        for j in range(sp - 1):
            leave(j)

        @pl.when(sec > 0)
        def _():
            filter_terms(m)

        @pl.when(is_last & (m + 1 < mb))
        def _():
            prep(jnp.minimum(m + 1, mb - 1))

        @pl.when(has_outer)
        def _():
            face_out(m).wait_recv()

        gbuf[m, sp - 1] = gbuf[m, sp - 1] + frecv[m, 1]
        leave(sp - 1)
        return carry

    lax.fori_loop(0, mb, step, 0)

    @pl.when(sec > 0)
    def _():
        pair().start()

    mine = pl.multiple_of(core * half, 8)
    pair().wait_recv()
    hbuf[...] = acc[pl.ds(mine, half), :] + pbuf[...]
    for p in range(pieces):
        for t in range(1, n2):
            scatter(p, t).start()
    for p in range(pieces):
        total = hbuf[pl.ds(pl.multiple_of(zed * rs + p * 8, 8), 8), :]
        for t in range(1, n2):
            scatter(p, t).wait_recv()
            total = total + cbuf[t - 1, p * 8 : (p + 1) * 8, :]
        full[rows_of(p, 0), :] = total * scale
        for t in range(1, n2):
            gather(p, t).start()
        forward(p, 0).start()
    for p in range(pieces):
        for t in range(1, n2):
            arrived(p, t).wait_recv()
            forward(p, t).start()
    for p in range(pieces):
        for t in range(n2):
            forward(p, t).wait_recv()
    for k in range(27):
        a, k9 = k // 9, k % 9
        fbuf[k] = full[a * ch : (a + 1) * ch, k9 * ch : (k9 + 1) * ch]
    fout = pltpu.make_async_copy(fbuf, fsum, fout_sem)
    fout.start()
    pair().wait_send()
    for p in range(pieces):
        for t in range(1, n2):
            scatter(p, t).wait_send()
            gather(p, t).wait_send()
        for t in range(n2):
            forward(p, t).wait_send()
    for m in range(mb):
        halo_in(m).wait_send()
        face_in(m).wait_send()
        for j in range(sp):
            out_copy(m, j).wait()

    @pl.when(has_outer)
    def _():
        for m in range(mb):
            halo_out(m).wait_send()
            face_out(m).wait_send()

    @pl.when(sec > 0)
    def _():
        for m in range(mb):
            for j in range(sp):
                hop(m, j).wait_send()

    fout.wait()


def per_device(n_sec, n_dep, activations, filters, cotangent):
    act, filt = activations[0], filters[0]
    mb, sp, ch, cells = act.shape
    scale = 1.0 / math.sqrt(mb * sp * n_dep * H * W)
    any_spec = pl.BlockSpec(memory_space=pl.ANY)
    hbm_spec = pl.BlockSpec(memory_space=pltpu.MemorySpace.HBM)
    n2 = n_dep // 2
    rs = 8 * pl.cdiv(3 * ch, 16 * n2)
    dma = pltpu.SemaphoreType.DMA
    grads, fsum = pl.pallas_call(
        functools.partial(kernel, n_sec, n_dep, scale),
        out_shape=(
            jax.ShapeDtypeStruct(act.shape, F32),
            jax.ShapeDtypeStruct(filt.shape, F32),
        ),
        in_specs=[hbm_spec] * 3,
        out_specs=(any_spec, any_spec),
        scratch_shapes=[
            pltpu.VMEM((mb, sp + 2, ch, cells), F32),
            pltpu.VMEM(filt.shape, F32),
            pltpu.VMEM((mb, sp, ch, cells), F32),
            pltpu.VMEM((mb, sp, ch, cells), F32),
            pltpu.VMEM((mb, sp, ch, cells), F32),
            pltpu.VMEM((mb, 2, ch, cells), F32),
            pltpu.VMEM((mb, 2, ch, cells), F32),
            pltpu.VMEM((mb, sp + 2, 9 * ch, cells), BF16),
            pltpu.VMEM((mb, sp + 2, 9 * ch, cells), BF16),
            pltpu.VMEM((sp, 9 * ch, cells), BF16),
            pltpu.VMEM((sp, 9 * ch, cells), BF16),
            pltpu.VMEM((6 * ch, 9 * ch), BF16),
            pltpu.VMEM((3 * ch, 9 * ch), BF16),
            pltpu.VMEM((6 * ch, 9 * ch), BF16),
            pltpu.VMEM((3 * ch, 9 * ch), BF16),
            pltpu.VMEM((2 * sp * ch, cells), BF16),
            pltpu.VMEM((sp * ch, cells), BF16),
            pltpu.VMEM((2 * n2 * rs, 9 * ch), F32),
            pltpu.VMEM((n2 * rs, 9 * ch), F32),
            pltpu.VMEM((n2 * rs, 9 * ch), F32),
            pltpu.VMEM((max(n2 - 1, 1), rs, 9 * ch), F32),
            pltpu.VMEM((2 * n2 * rs, 9 * ch), F32),
            dma((mb, sp)), dma, dma((mb, sp)),
            dma((2, mb)), dma((2, mb)), dma((2, mb)), dma((2, mb)),
            dma((mb, sp)), dma((mb, sp)), dma((mb, sp)),
            dma, dma, *[dma((rs // 8, n2))] * 6, dma,
        ],
        compiler_params=pltpu.CompilerParams(
            collective_id=0, has_side_effects=True, vmem_limit_bytes=60 * 1024 * 1024),
    )(act, filt, cotangent)
    return grads[None], fsum[None]


def solution(mesh):
    return jax.shard_map(
        functools.partial(per_device, mesh.shape["section"], mesh.shape["depth"]),
        mesh=mesh,
        in_specs=(
            P("section", None, "depth", None, None),
            P("section", None, None, None),
            P(None, "depth", None, None),
        ),
        out_specs=(P("section", None, "depth", None, None), P("section", None, None, None)),
        check_vma=False,
    )
```

```python
import functools
import math

import jax
import jax.numpy as jnp
from jax import lax
from jax.experimental import pallas as pl
from jax.experimental.pallas import tpu as pltpu
from jax.sharding import PartitionSpec as P

H = 16
W = 16
F32 = jnp.float32
BF16 = jnp.bfloat16
MESH = pl.DeviceIdType.MESH


def split(x):
    hi = x.astype(BF16)
    return hi, (x - hi.astype(F32)).astype(BF16)


def tap_masks(cells):
    lane = lax.broadcasted_iota(jnp.int32, (1, cells), 1)
    y, x = lane // W, lane % W
    masks = []
    for b in (-1, 0, 1):
        for c in (-1, 0, 1):
            masks.append((y + b >= 0) & (y + b < H) & (x + c >= 0) & (x + c < W))
    return masks


def put_patches(plane, hi_ref, lo_ref, masks):
    ch, cells = plane.shape
    for k in range(9):
        by = (k // 3 - 1) * W + (k % 3 - 1)
        v = plane if by == 0 else pltpu.roll(plane, (-by) % cells, 1)
        if by != 0:
            v = jnp.where(masks[k], v, 0.0)
        hi, lo = split(v)
        hi_ref[k * ch : (k + 1) * ch, :] = hi
        lo_ref[k * ch : (k + 1) * ch, :] = lo


def dot(a, b):
    return jnp.dot(a, b, preferred_element_type=F32)


def dot_nt(a, b):
    return lax.dot_general(a, b, (((1,), (1,)), ((), ())), preferred_element_type=F32)


def kernel(
    n_sec, n_dep, scale,
    act, filt, cot,
    grads, fsum,
    ext, fbuf, up, slope, gbuf, fsend, frecv,
    p_hi, p_lo, s_hi, s_lo, fs, fh, gs, gh, ss, sh, acc,
    pbuf, hbuf, cbuf, full,
    own_sem, filt_sem, cot_sem, halo_send, halo_recv, face_send, face_recv, hop_send, hop_recv, out_sem,
    pair_send, pair_recv, rs_send, rs_recv, ag_send, ag_recv, fw_send, fw_recv, fout_sem,
):
    mb, sp, ch, cells = act.shape
    sec, dep = lax.axis_index("section"), lax.axis_index("depth")
    n2 = n_dep // 2
    zed, core = dep // 2, dep % 2
    is_last = sec == n_sec - 1
    toward = 2 * core - 1
    outer_dep = dep + toward
    has_outer = (outer_dep >= 0) & (outer_dep < n_dep)
    partner, outside = (sec, dep - toward), (sec, outer_dep)
    masks = tap_masks(cells)

    def plane(j):
        return core * j + (1 - core) * (sp - 1 - j)

    def tap(a):
        return core * a + (1 - core) * (2 - a)

    def remote(src, dst, send, recv, target):
        return pltpu.make_async_remote_copy(src, dst, send, recv, device_id=target, device_id_type=MESH)

    def own_copy(m, j):
        return pltpu.make_async_copy(act.at[m, plane(j)], ext.at[m, j + 1], own_sem.at[m, j])

    def cot_copy(m, j):
        return pltpu.make_async_copy(cot.at[m, plane(j)], up.at[m, j], cot_sem.at[m, j])

    filt_copy = pltpu.make_async_copy(filt, fbuf, filt_sem)
    filt_copy.start()
    for m in range(mb):
        for j in range(sp):
            own_copy(m, j).start()

    @pl.when(is_last)
    def _():
        for m in range(mb):
            for j in range(sp):
                cot_copy(m, j).start()

    half = acc.shape[0] // 2
    rs = half // n2
    pieces = rs // 8

    def peer(t):
        return (sec, ((zed + t) % n2) * 2 + core)

    barrier = pltpu.get_barrier_semaphore()
    for target in (
        (sec, (dep + 1) % n_dep), (sec, (dep + n_dep - 1) % n_dep),
        ((sec + 1) % n_sec, dep), ((sec + n_sec - 1) % n_sec, dep),
        *(peer(t) for t in range(1, n2)),
    ):
        pl.semaphore_signal(barrier, inc=1, device_id=target, device_id_type=MESH)
    pl.semaphore_wait(barrier, 3 + n2)

    def halo_in(m):
        return remote(act.at[m, plane(0)], ext.at[m, 0], halo_send.at[0, m], halo_recv.at[0, m], partner)

    def halo_out(m):
        return remote(act.at[m, plane(sp - 1)], ext.at[m, sp + 1], halo_send.at[1, m], halo_recv.at[1, m], outside)

    def face_in(m):
        return remote(fsend.at[m, 0], frecv.at[m, 0], face_send.at[0, m], face_recv.at[0, m], partner)

    def face_out(m):
        return remote(fsend.at[m, 1], frecv.at[m, 1], face_send.at[1, m], face_recv.at[1, m], outside)

    def hop(m, j):
        return remote(gbuf.at[m, j], up.at[m, j], hop_send.at[m, j], hop_recv.at[m, j], (sec - 1, dep))

    def out_copy(m, j):
        return pltpu.make_async_copy(gbuf.at[m, j], grads.at[m, plane(j)], out_sem.at[m, j])

    def pair():
        theirs = pl.multiple_of((1 - core) * half, 8)
        return remote(acc.at[pl.ds(theirs, half)], pbuf, pair_send, pair_recv, partner)

    def scatter(p, t):
        rows = pl.ds(pl.multiple_of(((zed + t) % n2) * rs + p * 8, 8), 8)
        return remote(hbuf.at[rows], cbuf.at[t - 1, pl.ds(p * 8, 8)], rs_send.at[p, t - 1], rs_recv.at[p, t - 1], peer(t))

    def rows_of(p, t):
        return pl.ds(pl.multiple_of(core * half + ((zed + n2 - t) % n2) * rs + p * 8, 8), 8)

    def gather(p, t):
        rows = rows_of(p, 0)
        return remote(full.at[rows], full.at[rows], ag_send.at[p, t - 1], ag_recv.at[p, t - 1], peer(t))

    def arrived(p, t):
        rows = rows_of(p, t)
        return remote(full.at[rows], full.at[rows], ag_send.at[p, t - 1], ag_recv.at[p, t - 1], peer(t))

    def forward(p, t):
        rows = rows_of(p, t)
        return remote(full.at[rows], full.at[rows], fw_send.at[p, t], fw_recv.at[p, t], partner)

    @pl.when(has_outer)
    def _():
        for m in range(mb):
            halo_out(m).start()

    for m in range(mb):
        halo_in(m).start()

    @pl.when(jnp.logical_not(has_outer))
    def _():
        for m in range(mb):
            ext[m, sp + 1] = jnp.zeros((ch, cells), F32)
            frecv[m, 1] = jnp.zeros((ch, cells), F32)

    filt_copy.wait()
    for a in range(3):
        r = tap(a)
        two, one = pl.multiple_of(2 * r * ch, 2 * ch), pl.multiple_of(r * ch, ch)
        for k9 in range(9):
            w = fbuf[9 * a + k9]
            hi, lo = split(w)
            cols = slice(k9 * ch, (k9 + 1) * ch)
            fs[pl.ds(two, ch), cols] = hi
            fs[pl.ds(two + ch, ch), cols] = lo
            fh[pl.ds(one, ch), cols] = hi
            hi, lo = split(w.T)
            cols = slice((8 - k9) * ch, (9 - k9) * ch)
            gs[pl.ds(two, ch), cols] = hi
            gs[pl.ds(two + ch, ch), cols] = lo
            gh[pl.ds(one, ch), cols] = hi
    acc[...] = jnp.zeros_like(acc)

    def taps_of(e):
        return max(0, e - (sp - 1)), min(2, e)

    def parts(yh, yl, n):
        return [
            yh[2 * i * ch : (2 * i + 1) * ch] + yh[(2 * i + 1) * ch : (2 * i + 2) * ch] + yl[i * ch : (i + 1) * ch]
            for i in range(n)
        ]

    def prep(m):
        pre = [None] * sp
        for e in [*range(1, sp + 1), 0, sp + 1]:
            if e == 0:
                halo_in(m).wait_recv()
            elif e <= sp:
                own_copy(m, e - 1).wait()
            else:
                @pl.when(has_outer)
                def _():
                    halo_out(m).wait_recv()
            hi_ref, lo_ref = p_hi.at[m, e], p_lo.at[m, e]
            put_patches(ext[m, e], hi_ref, lo_ref, masks)
            a0, a1 = taps_of(e)
            yh = dot(fs[2 * a0 * ch : 2 * (a1 + 1) * ch, :], hi_ref[...])
            yl = dot(fh[a0 * ch : (a1 + 1) * ch, :], lo_ref[...])
            for i, part in enumerate(parts(yh, yl, a1 - a0 + 1)):
                d = e - a0 - i
                pre[d] = part if pre[d] is None else pre[d] + part
        for d in range(sp):
            sg = jax.nn.sigmoid(pre[d])
            slope[m, d] = sg * (1.0 + pre[d] * (1.0 - sg))

    def back(d, a0, a1):
        yh = dot(gs[2 * a0 * ch : 2 * (a1 + 1) * ch, :], s_hi[d])
        yl = dot(gh[a0 * ch : (a1 + 1) * ch, :], s_lo[d])
        return parts(yh, yl, a1 - a0 + 1)

    def filter_terms(m):
        for e in range(sp + 2):
            a0, a1 = taps_of(e)
            r0 = sp - 1 - (e - a0)
            n = a1 - a0 + 1
            yh = dot_nt(ss[2 * r0 * ch : 2 * (r0 + n) * ch, :], p_hi[m, e])
            yl = dot_nt(sh[r0 * ch : (r0 + n) * ch, :], p_lo[m, e])
            for i, part in enumerate(parts(yh, yl, n)):
                rows = pl.ds(pl.multiple_of(tap(a0 + i) * ch, ch), ch)
                acc[rows, :] += part

    prep(0)

    @pl.when(jnp.logical_not(is_last))
    def _():
        def more(m, carry):
            prep(m)
            return carry
        lax.fori_loop(1, mb, more, 0)

    def cotangents(m, d):
        @pl.when(is_last)
        def _():
            cot_copy(m, d).wait()

        @pl.when(jnp.logical_not(is_last))
        def _():
            hop(m, d).wait_recv()

        s = up[m, d] * slope[m, d]
        hi, lo = split(s)
        r = sp - 1 - d
        ss[2 * r * ch : (2 * r + 1) * ch, :] = hi
        ss[(2 * r + 1) * ch : (2 * r + 2) * ch, :] = lo
        sh[r * ch : (r + 1) * ch, :] = hi
        put_patches(s, s_hi.at[d], s_lo.at[d], masks)

    def inner(m):
        cotangents(m, 0)
        fsend[m, 0] = back(0, 0, 0)[0]
        face_in(m).start()

    inner(0)

    def step(m, carry):
        def leave(j):
            @pl.when(sec > 0)
            def _():
                hop(m, j).start()

            out_copy(m, j).start()

        for d in range(1, sp):
            cotangents(m, d)
        fsend[m, 1] = back(sp - 1, 2, 2)[0]

        @pl.when(has_outer)
        def _():
            face_out(m).start()

        @pl.when(sec == 0)
        def _():
            filter_terms(m)

        @pl.when((sec == 0) & (m == mb - 1))
        def _():
            pair().start()

        out = [None] * sp
        for d in range(sp):
            a0 = 1 if d == 0 else 0
            a1 = 1 if d == sp - 1 else 2
            for i, part in enumerate(back(d, a0, a1)):
                o = d + a0 + i - 1
                out[o] = part if out[o] is None else out[o] + part
        for d in range(1, sp):
            gbuf[m, d] = out[d]
        face_in(m).wait_recv()
        gbuf[m, 0] = out[0] + frecv[m, 0]
        for j in range(sp - 1):
            leave(j)

        @pl.when(sec > 0)
        def _():
            filter_terms(m)

        @pl.when(is_last & (m + 1 < mb))
        def _():
            prep(jnp.minimum(m + 1, mb - 1))

        @pl.when(m + 1 < mb)
        def _():
            inner(jnp.minimum(m + 1, mb - 1))

        @pl.when(has_outer)
        def _():
            face_out(m).wait_recv()

        gbuf[m, sp - 1] = gbuf[m, sp - 1] + frecv[m, 1]
        leave(sp - 1)
        return carry

    lax.fori_loop(0, mb, step, 0)

    @pl.when(sec > 0)
    def _():
        pair().start()

    mine = pl.multiple_of(core * half, 8)
    pair().wait_recv()
    hbuf[...] = acc[pl.ds(mine, half), :] + pbuf[...]
    for p in range(pieces):
        for t in range(1, n2):
            scatter(p, t).start()
    for p in range(pieces):
        total = hbuf[pl.ds(pl.multiple_of(zed * rs + p * 8, 8), 8), :]
        for t in range(1, n2):
            scatter(p, t).wait_recv()
            total = total + cbuf[t - 1, p * 8 : (p + 1) * 8, :]
        full[rows_of(p, 0), :] = total * scale
        for t in range(1, n2):
            gather(p, t).start()
        forward(p, 0).start()
    for p in range(pieces):
        for t in range(1, n2):
            arrived(p, t).wait_recv()
            forward(p, t).start()
    for p in range(pieces):
        for t in range(n2):
            forward(p, t).wait_recv()
    for k in range(27):
        a, k9 = k // 9, k % 9
        fbuf[k] = full[a * ch : (a + 1) * ch, k9 * ch : (k9 + 1) * ch]
    fout = pltpu.make_async_copy(fbuf, fsum, fout_sem)
    fout.start()
    pair().wait_send()
    for p in range(pieces):
        for t in range(1, n2):
            scatter(p, t).wait_send()
            gather(p, t).wait_send()
        for t in range(n2):
            forward(p, t).wait_send()
    for m in range(mb):
        halo_in(m).wait_send()
        face_in(m).wait_send()
        for j in range(sp):
            out_copy(m, j).wait()

    @pl.when(has_outer)
    def _():
        for m in range(mb):
            halo_out(m).wait_send()
            face_out(m).wait_send()

    @pl.when(sec > 0)
    def _():
        for m in range(mb):
            for j in range(sp):
                hop(m, j).wait_send()

    fout.wait()


def per_device(n_sec, n_dep, activations, filters, cotangent):
    act, filt = activations[0], filters[0]
    mb, sp, ch, cells = act.shape
    scale = 1.0 / math.sqrt(mb * sp * n_dep * H * W)
    any_spec = pl.BlockSpec(memory_space=pl.ANY)
    hbm_spec = pl.BlockSpec(memory_space=pltpu.MemorySpace.HBM)
    n2 = n_dep // 2
    rs = 8 * pl.cdiv(3 * ch, 16 * n2)
    dma = pltpu.SemaphoreType.DMA
    grads, fsum = pl.pallas_call(
        functools.partial(kernel, n_sec, n_dep, scale),
        out_shape=(
            jax.ShapeDtypeStruct(act.shape, F32),
            jax.ShapeDtypeStruct(filt.shape, F32),
        ),
        in_specs=[hbm_spec] * 3,
        out_specs=(any_spec, any_spec),
        scratch_shapes=[
            pltpu.VMEM((mb, sp + 2, ch, cells), F32),
            pltpu.VMEM(filt.shape, F32),
            pltpu.VMEM((mb, sp, ch, cells), F32),
            pltpu.VMEM((mb, sp, ch, cells), F32),
            pltpu.VMEM((mb, sp, ch, cells), F32),
            pltpu.VMEM((mb, 2, ch, cells), F32),
            pltpu.VMEM((mb, 2, ch, cells), F32),
            pltpu.VMEM((mb, sp + 2, 9 * ch, cells), BF16),
            pltpu.VMEM((mb, sp + 2, 9 * ch, cells), BF16),
            pltpu.VMEM((sp, 9 * ch, cells), BF16),
            pltpu.VMEM((sp, 9 * ch, cells), BF16),
            pltpu.VMEM((6 * ch, 9 * ch), BF16),
            pltpu.VMEM((3 * ch, 9 * ch), BF16),
            pltpu.VMEM((6 * ch, 9 * ch), BF16),
            pltpu.VMEM((3 * ch, 9 * ch), BF16),
            pltpu.VMEM((2 * sp * ch, cells), BF16),
            pltpu.VMEM((sp * ch, cells), BF16),
            pltpu.VMEM((2 * n2 * rs, 9 * ch), F32),
            pltpu.VMEM((n2 * rs, 9 * ch), F32),
            pltpu.VMEM((n2 * rs, 9 * ch), F32),
            pltpu.VMEM((max(n2 - 1, 1), rs, 9 * ch), F32),
            pltpu.VMEM((2 * n2 * rs, 9 * ch), F32),
            dma((mb, sp)), dma, dma((mb, sp)),
            dma((2, mb)), dma((2, mb)), dma((2, mb)), dma((2, mb)),
            dma((mb, sp)), dma((mb, sp)), dma((mb, sp)),
            dma, dma, *[dma((rs // 8, n2))] * 6, dma,
        ],
        compiler_params=pltpu.CompilerParams(
            collective_id=0, has_side_effects=True, vmem_limit_bytes=60 * 1024 * 1024),
    )(act, filt, cotangent)
    return grads[None], fsum[None]


def solution(mesh):
    return jax.shard_map(
        functools.partial(per_device, mesh.shape["section"], mesh.shape["depth"]),
        mesh=mesh,
        in_specs=(
            P("section", None, "depth", None, None),
            P("section", None, None, None),
            P(None, "depth", None, None),
        ),
        out_specs=(P("section", None, "depth", None, None), P("section", None, None, None)),
        check_vma=False,
    )
```

```python
import functools
import math

import jax
import jax.numpy as jnp
from jax import lax
from jax.experimental import pallas as pl
from jax.experimental.pallas import tpu as pltpu
from jax.sharding import PartitionSpec as P

H = 16
W = 16
F32 = jnp.float32
BF16 = jnp.bfloat16
MESH = pl.DeviceIdType.MESH


def split(x):
    hi = x.astype(BF16)
    return hi, (x - hi.astype(F32)).astype(BF16)


def tap_masks(cells):
    lane = lax.broadcasted_iota(jnp.int32, (1, cells), 1)
    y, x = lane // W, lane % W
    masks = []
    for b in (-1, 0, 1):
        for c in (-1, 0, 1):
            masks.append((y + b >= 0) & (y + b < H) & (x + c >= 0) & (x + c < W))
    return masks


def put_patches(plane, hi_ref, lo_ref, masks):
    ch, cells = plane.shape
    for k in range(9):
        by = (k // 3 - 1) * W + (k % 3 - 1)
        v = plane if by == 0 else pltpu.roll(plane, (-by) % cells, 1)
        if by != 0:
            v = jnp.where(masks[k], v, 0.0)
        hi, lo = split(v)
        hi_ref[k * ch : (k + 1) * ch, :] = hi
        lo_ref[k * ch : (k + 1) * ch, :] = lo


def dot(a, b):
    return jnp.dot(a, b, preferred_element_type=F32)


def dot_nt(a, b):
    return lax.dot_general(a, b, (((1,), (1,)), ((), ())), preferred_element_type=F32)


def kernel(
    n_sec, n_dep, scale,
    act, filt, cot,
    grads, fsum,
    ext, fbuf, up, slope, gbuf, fsend, frecv,
    p_hi, p_lo, s_hi, s_lo, fs, fh, gs, gh, ss, sh, acc,
    pbuf, hbuf, cbuf, full,
    own_sem, filt_sem, cot_sem, halo_send, halo_recv, face_send, face_recv, hop_send, hop_recv, out_sem,
    pair_send, pair_recv, rs_send, rs_recv, ag_send, ag_recv, fw_send, fw_recv, fout_sem,
):
    mb, sp, ch, cells = act.shape
    sec, dep = lax.axis_index("section"), lax.axis_index("depth")
    n2 = n_dep // 2
    zed, core = dep // 2, dep % 2
    is_last = sec == n_sec - 1
    toward = 2 * core - 1
    outer_dep = dep + toward
    has_outer = (outer_dep >= 0) & (outer_dep < n_dep)
    partner, outside = (sec, dep - toward), (sec, outer_dep)
    masks = tap_masks(cells)

    def plane(j):
        return core * j + (1 - core) * (sp - 1 - j)

    def tap(a):
        return core * a + (1 - core) * (2 - a)

    def remote(src, dst, send, recv, target):
        return pltpu.make_async_remote_copy(src, dst, send, recv, device_id=target, device_id_type=MESH)

    def own_copy(m, j):
        return pltpu.make_async_copy(act.at[m, plane(j)], ext.at[m, j + 1], own_sem.at[m, j])

    def cot_copy(m, j):
        return pltpu.make_async_copy(cot.at[m, plane(j)], up.at[m, j], cot_sem.at[m, j])

    filt_copy = pltpu.make_async_copy(filt, fbuf, filt_sem)
    filt_copy.start()
    for m in range(mb):
        for j in range(sp):
            own_copy(m, j).start()

    @pl.when(is_last)
    def _():
        for m in range(mb):
            for j in range(sp):
                cot_copy(m, j).start()

    half = acc.shape[0] // 2
    rs = half // n2
    pieces = rs // 8

    def peer(t):
        return (sec, ((zed + t) % n2) * 2 + core)

    barrier = pltpu.get_barrier_semaphore()
    for target in (
        (sec, (dep + 1) % n_dep), (sec, (dep + n_dep - 1) % n_dep),
        ((sec + 1) % n_sec, dep), ((sec + n_sec - 1) % n_sec, dep),
        *(peer(t) for t in range(1, n2)),
    ):
        pl.semaphore_signal(barrier, inc=1, device_id=target, device_id_type=MESH)
    pl.semaphore_wait(barrier, 3 + n2)

    def halo_in(m):
        return remote(act.at[m, plane(0)], ext.at[m, 0], halo_send.at[0, m], halo_recv.at[0, m], partner)

    def halo_out(m):
        return remote(act.at[m, plane(sp - 1)], ext.at[m, sp + 1], halo_send.at[1, m], halo_recv.at[1, m], outside)

    def face_in(m):
        return remote(fsend.at[m, 0], frecv.at[m, 0], face_send.at[0, m], face_recv.at[0, m], partner)

    def face_out(m):
        return remote(fsend.at[m, 1], frecv.at[m, 1], face_send.at[1, m], face_recv.at[1, m], outside)

    def hop(m, j):
        return remote(gbuf.at[m, j], up.at[m, j], hop_send.at[m, j], hop_recv.at[m, j], (sec - 1, dep))

    def out_copy(m, j):
        return pltpu.make_async_copy(gbuf.at[m, j], grads.at[m, plane(j)], out_sem.at[m, j])

    def pair():
        theirs = pl.multiple_of((1 - core) * half, 8)
        return remote(acc.at[pl.ds(theirs, half)], pbuf, pair_send, pair_recv, partner)

    def scatter(p, t):
        rows = pl.ds(pl.multiple_of(((zed + t) % n2) * rs + p * 8, 8), 8)
        return remote(hbuf.at[rows], cbuf.at[t - 1, pl.ds(p * 8, 8)], rs_send.at[p, t - 1], rs_recv.at[p, t - 1], peer(t))

    def rows_of(p, t):
        return pl.ds(pl.multiple_of(core * half + ((zed + n2 - t) % n2) * rs + p * 8, 8), 8)

    def gather(p, t):
        rows = rows_of(p, 0)
        return remote(full.at[rows], full.at[rows], ag_send.at[p, t - 1], ag_recv.at[p, t - 1], peer(t))

    def arrived(p, t):
        rows = rows_of(p, t)
        return remote(full.at[rows], full.at[rows], ag_send.at[p, t - 1], ag_recv.at[p, t - 1], peer(t))

    def forward(p, t):
        rows = rows_of(p, t)
        return remote(full.at[rows], full.at[rows], fw_send.at[p, t], fw_recv.at[p, t], partner)

    @pl.when(has_outer)
    def _():
        for m in range(mb):
            halo_out(m).start()

    for m in range(mb):
        halo_in(m).start()

    @pl.when(jnp.logical_not(has_outer))
    def _():
        for m in range(mb):
            ext[m, sp + 1] = jnp.zeros((ch, cells), F32)
            frecv[m, 1] = jnp.zeros((ch, cells), F32)

    filt_copy.wait()
    for a in range(3):
        r = tap(a)
        two, one = pl.multiple_of(2 * r * ch, 2 * ch), pl.multiple_of(r * ch, ch)
        for k9 in range(9):
            w = fbuf[9 * a + k9]
            hi, lo = split(w)
            cols = slice(k9 * ch, (k9 + 1) * ch)
            fs[pl.ds(two, ch), cols] = hi
            fs[pl.ds(two + ch, ch), cols] = lo
            fh[pl.ds(one, ch), cols] = hi
            hi, lo = split(w.T)
            cols = slice((8 - k9) * ch, (9 - k9) * ch)
            gs[pl.ds(two, ch), cols] = hi
            gs[pl.ds(two + ch, ch), cols] = lo
            gh[pl.ds(one, ch), cols] = hi
    acc[...] = jnp.zeros_like(acc)

    def taps_of(e):
        return max(0, e - (sp - 1)), min(2, e)

    def parts(yh, yl, n):
        return [
            yh[2 * i * ch : (2 * i + 1) * ch] + yh[(2 * i + 1) * ch : (2 * i + 2) * ch] + yl[i * ch : (i + 1) * ch]
            for i in range(n)
        ]

    def prep(m):
        pre = [None] * sp
        for e in [*range(1, sp + 1), 0, sp + 1]:
            if e == 0:
                halo_in(m).wait_recv()
            elif e <= sp:
                own_copy(m, e - 1).wait()
            else:
                @pl.when(has_outer)
                def _():
                    halo_out(m).wait_recv()
            hi_ref, lo_ref = p_hi.at[m, e], p_lo.at[m, e]
            put_patches(ext[m, e], hi_ref, lo_ref, masks)
            a0, a1 = taps_of(e)
            yh = dot(fs[2 * a0 * ch : 2 * (a1 + 1) * ch, :], hi_ref[...])
            yl = dot(fh[a0 * ch : (a1 + 1) * ch, :], lo_ref[...])
            for i, part in enumerate(parts(yh, yl, a1 - a0 + 1)):
                d = e - a0 - i
                pre[d] = part if pre[d] is None else pre[d] + part
        for d in range(sp):
            sg = jax.nn.sigmoid(pre[d])
            slope[m, d] = sg * (1.0 + pre[d] * (1.0 - sg))

    def back(d, a0, a1):
        yh = dot(gs[2 * a0 * ch : 2 * (a1 + 1) * ch, :], s_hi[d])
        yl = dot(gh[a0 * ch : (a1 + 1) * ch, :], s_lo[d])
        return parts(yh, yl, a1 - a0 + 1)

    def filter_terms(m):
        for e in range(sp + 2):
            a0, a1 = taps_of(e)
            r0 = sp - 1 - (e - a0)
            n = a1 - a0 + 1
            yh = dot_nt(ss[2 * r0 * ch : 2 * (r0 + n) * ch, :], p_hi[m, e])
            yl = dot_nt(sh[r0 * ch : (r0 + n) * ch, :], p_lo[m, e])
            for i, part in enumerate(parts(yh, yl, n)):
                rows = pl.ds(pl.multiple_of(tap(a0 + i) * ch, ch), ch)
                acc[rows, :] += part

    prep(0)

    @pl.when(jnp.logical_not(is_last))
    def _():
        def more(m, carry):
            prep(m)
            return carry
        lax.fori_loop(1, mb, more, 0)

    def cotangents(m, d):
        @pl.when(is_last)
        def _():
            cot_copy(m, d).wait()

        @pl.when(jnp.logical_not(is_last))
        def _():
            hop(m, d).wait_recv()

        s = up[m, d] * slope[m, d]
        hi, lo = split(s)
        r = sp - 1 - d
        ss[2 * r * ch : (2 * r + 1) * ch, :] = hi
        ss[(2 * r + 1) * ch : (2 * r + 2) * ch, :] = lo
        sh[r * ch : (r + 1) * ch, :] = hi
        put_patches(s, s_hi.at[d], s_lo.at[d], masks)

    def inner(m):
        cotangents(m, 0)
        fsend[m, 0] = back(0, 0, 0)[0]
        face_in(m).start()

    inner(0)

    def step(m, carry):
        def leave(j):
            @pl.when(sec > 0)
            def _():
                hop(m, j).start()

            out_copy(m, j).start()

        for d in range(1, sp):
            cotangents(m, d)
        fsend[m, 1] = back(sp - 1, 2, 2)[0]

        @pl.when(has_outer)
        def _():
            face_out(m).start()

        @pl.when(sec == 0)
        def _():
            filter_terms(m)

        @pl.when((sec == 0) & (m == mb - 1))
        def _():
            pair().start()

        out = [None] * sp
        for d in range(sp):
            a0 = 1 if d == 0 else 0
            a1 = 1 if d == sp - 1 else 2
            for i, part in enumerate(back(d, a0, a1)):
                o = d + a0 + i - 1
                out[o] = part if out[o] is None else out[o] + part
        for d in range(1, sp):
            gbuf[m, d] = out[d]
        face_in(m).wait_recv()
        gbuf[m, 0] = out[0] + frecv[m, 0]
        for j in range(sp - 1):
            leave(j)

        @pl.when(sec > 0)
        def _():
            filter_terms(m)

        @pl.when(is_last & (m + 1 < mb))
        def _():
            prep(jnp.minimum(m + 1, mb - 1))

        @pl.when(is_last & (m + 1 < mb))
        def _():
            inner(jnp.minimum(m + 1, mb - 1))

        @pl.when(has_outer)
        def _():
            face_out(m).wait_recv()

        gbuf[m, sp - 1] = gbuf[m, sp - 1] + frecv[m, 1]
        leave(sp - 1)

        @pl.when(jnp.logical_not(is_last) & (m + 1 < mb))
        def _():
            inner(jnp.minimum(m + 1, mb - 1))

        return carry

    lax.fori_loop(0, mb, step, 0)

    @pl.when(sec > 0)
    def _():
        pair().start()

    mine = pl.multiple_of(core * half, 8)
    pair().wait_recv()
    hbuf[...] = acc[pl.ds(mine, half), :] + pbuf[...]
    for p in range(pieces):
        for t in range(1, n2):
            scatter(p, t).start()
    for p in range(pieces):
        total = hbuf[pl.ds(pl.multiple_of(zed * rs + p * 8, 8), 8), :]
        for t in range(1, n2):
            scatter(p, t).wait_recv()
            total = total + cbuf[t - 1, p * 8 : (p + 1) * 8, :]
        full[rows_of(p, 0), :] = total * scale
        for t in range(1, n2):
            gather(p, t).start()
        forward(p, 0).start()
    for p in range(pieces):
        for t in range(1, n2):
            arrived(p, t).wait_recv()
            forward(p, t).start()
    for p in range(pieces):
        for t in range(n2):
            forward(p, t).wait_recv()
    for k in range(27):
        a, k9 = k // 9, k % 9
        fbuf[k] = full[a * ch : (a + 1) * ch, k9 * ch : (k9 + 1) * ch]
    fout = pltpu.make_async_copy(fbuf, fsum, fout_sem)
    fout.start()
    pair().wait_send()
    for p in range(pieces):
        for t in range(1, n2):
            scatter(p, t).wait_send()
            gather(p, t).wait_send()
        for t in range(n2):
            forward(p, t).wait_send()
    for m in range(mb):
        halo_in(m).wait_send()
        face_in(m).wait_send()
        for j in range(sp):
            out_copy(m, j).wait()

    @pl.when(has_outer)
    def _():
        for m in range(mb):
            halo_out(m).wait_send()
            face_out(m).wait_send()

    @pl.when(sec > 0)
    def _():
        for m in range(mb):
            for j in range(sp):
                hop(m, j).wait_send()

    fout.wait()


def per_device(n_sec, n_dep, activations, filters, cotangent):
    act, filt = activations[0], filters[0]
    mb, sp, ch, cells = act.shape
    scale = 1.0 / math.sqrt(mb * sp * n_dep * H * W)
    any_spec = pl.BlockSpec(memory_space=pl.ANY)
    hbm_spec = pl.BlockSpec(memory_space=pltpu.MemorySpace.HBM)
    n2 = n_dep // 2
    rs = 8 * pl.cdiv(3 * ch, 16 * n2)
    dma = pltpu.SemaphoreType.DMA
    grads, fsum = pl.pallas_call(
        functools.partial(kernel, n_sec, n_dep, scale),
        out_shape=(
            jax.ShapeDtypeStruct(act.shape, F32),
            jax.ShapeDtypeStruct(filt.shape, F32),
        ),
        in_specs=[hbm_spec] * 3,
        out_specs=(any_spec, any_spec),
        scratch_shapes=[
            pltpu.VMEM((mb, sp + 2, ch, cells), F32),
            pltpu.VMEM(filt.shape, F32),
            pltpu.VMEM((mb, sp, ch, cells), F32),
            pltpu.VMEM((mb, sp, ch, cells), F32),
            pltpu.VMEM((mb, sp, ch, cells), F32),
            pltpu.VMEM((mb, 2, ch, cells), F32),
            pltpu.VMEM((mb, 2, ch, cells), F32),
            pltpu.VMEM((mb, sp + 2, 9 * ch, cells), BF16),
            pltpu.VMEM((mb, sp + 2, 9 * ch, cells), BF16),
            pltpu.VMEM((sp, 9 * ch, cells), BF16),
            pltpu.VMEM((sp, 9 * ch, cells), BF16),
            pltpu.VMEM((6 * ch, 9 * ch), BF16),
            pltpu.VMEM((3 * ch, 9 * ch), BF16),
            pltpu.VMEM((6 * ch, 9 * ch), BF16),
            pltpu.VMEM((3 * ch, 9 * ch), BF16),
            pltpu.VMEM((2 * sp * ch, cells), BF16),
            pltpu.VMEM((sp * ch, cells), BF16),
            pltpu.VMEM((2 * n2 * rs, 9 * ch), F32),
            pltpu.VMEM((n2 * rs, 9 * ch), F32),
            pltpu.VMEM((n2 * rs, 9 * ch), F32),
            pltpu.VMEM((max(n2 - 1, 1), rs, 9 * ch), F32),
            pltpu.VMEM((2 * n2 * rs, 9 * ch), F32),
            dma((mb, sp)), dma, dma((mb, sp)),
            dma((2, mb)), dma((2, mb)), dma((2, mb)), dma((2, mb)),
            dma((mb, sp)), dma((mb, sp)), dma((mb, sp)),
            dma, dma, *[dma((rs // 8, n2))] * 6, dma,
        ],
        compiler_params=pltpu.CompilerParams(
            collective_id=0, has_side_effects=True, vmem_limit_bytes=54000 * 1024),
    )(act, filt, cotangent)
    return grads[None], fsum[None]


def solution(mesh):
    return jax.shard_map(
        functools.partial(per_device, mesh.shape["section"], mesh.shape["depth"]),
        mesh=mesh,
        in_specs=(
            P("section", None, "depth", None, None),
            P("section", None, None, None),
            P(None, "depth", None, None),
        ),
        out_specs=(P("section", None, "depth", None, None), P("section", None, None, None)),
        check_vma=False,
    )
```
